32 devices in a mesh: wide: 8 (over z, x), narrow: 4 (over y, core).
Axes of the slice: x: 2, y: 2, z: 4, core: 2. Of those that a mesh axis runs over, the one named last changes fastest.
Arguments:
- hidden: bfloat16 [512, 4, 8192], P('narrow', None, 'wide'), may hold values from -0.1796875 to 0.1796875
- grad_out: bfloat16 [512, 8192], P('narrow', 'wide'), may hold values from -6 to 6
- weight_base: bfloat16 [32768, 8192], P('narrow', 'wide'), may hold values from -0.0625 to 0.0625
- block_scale: bfloat16 [2048, 512], P('narrow', 'wide'), may hold values from 0.25 to 4
Outputs:
- grad_hidden: bfloat16 [512, 4, 8192], P('narrow', None, 'wide')
- grad_weight: bfloat16 [8192, 4, 8192], P('narrow', None, 'wide')
The draws below stay inside these ranges and needn't reach their ends.
All inputs are finite; a program needn't handle non-finite values.
Results may differ from the reference program's by a relative error of at most 0.0049.
Values may be sent and summed in bfloat16 or wider, within the bound.
A program may use at most 512 MiB of HBM per device.

```python
import math
import jax
import jax.numpy as jnp

D = 8192
FF = 32768
BLOCK = 16
TOKENS = 512
GROUPS = 4
FGROUP = 8192


def shard_levels(rng, extent, pieces, least, largest):
    def one(dim, shards_of):
        heights = jax.random.uniform(jax.random.fold_in(jax.random.fold_in(rng, 6), dim), (shards_of,), jnp.float32, least / len(pieces), largest / len(pieces))
        return jnp.repeat(jnp.exp(heights), extent[dim] // shards_of).reshape((-1,) + (1,) * (len(extent) - dim - 1))

    loudness = one(*pieces[0])
    for cut in pieces[1:]:
        loudness = loudness * one(*cut)
    return loudness


def noise(own_key, extent, deviation, reach, cuts=(), dtype=jnp.bfloat16):
    loudness = shard_levels(own_key, extent, cuts, -0.22, 0.18) if cuts else 1.0
    entries = jax.random.normal(own_key, extent, jnp.float32) * deviation * loudness
    return jnp.minimum(jnp.maximum(entries, -reach), reach).astype(dtype)


def setup_inputs(seed: int = 0) -> dict:
    streams_of = jax.random.split(jax.random.key(seed), 5)
    return {
        "hidden": noise(streams_of[0], (TOKENS, GROUPS, FGROUP), 0.03, 0.1796875, ((0, 4), (2, 8))),
        "grad_out": noise(streams_of[1], (TOKENS, D), 1.0, 6.0, ((0, 4), (1, 8))),
        "weight_base": noise(streams_of[2], (FF, D), D ** -0.5, 0.0625, ((0, 4), (1, 8))),
        "block_scale": jnp.clip(jnp.exp(math.log(4.0) - 2.7725887 * jax.random.uniform(streams_of[3], (FF // BLOCK, D // BLOCK), jnp.float32) ** shard_levels(streams_of[3], (FF // BLOCK, D // BLOCK), ((0, 4), (1, 8)), -0.2, 0.2)), 0.25, 4.0).astype(jnp.bfloat16),
    }


def apply_scales(values, scales):
    height, breadth = values.shape
    widened = jnp.repeat(scales, 16, axis=1).astype(jnp.float32)
    blocked = values.reshape(height // 16, 16, breadth).astype(jnp.float32)
    blocked = blocked * widened[:, None, :]
    return blocked.reshape(height, breadth).astype(jnp.bfloat16)


def reference(hidden, grad_out, weight_base, block_scale):
    effective = apply_scales(weight_base, block_scale)
    flat_hidden = hidden.reshape(hidden.shape[0], hidden.shape[1] * hidden.shape[2])
    grad_flat = jnp.dot(grad_out, effective.T, preferred_element_type=jnp.float32)
    grad_hidden = grad_flat.astype(jnp.bfloat16).reshape(hidden.shape)
    grad_weight = jnp.dot(grad_out.T, flat_hidden, preferred_element_type=jnp.float32)
    grad_weight = grad_weight.astype(jnp.bfloat16).reshape(grad_out.shape[1], hidden.shape[1], hidden.shape[2])
    return grad_hidden, grad_weight
```

```python
import jax
import jax.numpy as jnp
from jax import lax
from jax.sharding import PartitionSpec as P

RING_SIGN = 1
RING_ROWS = 4


def apply_scales(values, scales):
    height, breadth = values.shape
    widened = jnp.repeat(scales, 16, axis=1).astype(jnp.float32)
    blocked = values.reshape(height // 16, 16, breadth).astype(jnp.float32)
    blocked = blocked * widened[:, None, :]
    return blocked.reshape(height, breadth).astype(jnp.bfloat16)


def ring_order(size):
    return list(range(0, size, 2)) + list(range(1, size, 2))[::-1]


def ring_reduce_scatter(partial, size, width):
    order = ring_order(size)
    place = [0] * size
    for position, index in enumerate(order):
        place[index] = position
    me = jnp.asarray(place, jnp.int32)[lax.axis_index("wide")]
    order_table = jnp.asarray(order, jnp.int32)
    pairs = [(order[p], order[(p + RING_SIGN) % size]) for p in range(size)]

    def chunk(step):
        target = order_table[(me - RING_SIGN * (1 + step)) % size]
        return lax.dynamic_slice_in_dim(partial, target * width, width, 1)

    total = chunk(0)
    for step in range(1, size):
        arrived = lax.ppermute(total.astype(jnp.bfloat16), "wide", pairs)
        total = arrived.astype(jnp.float32) + chunk(step)
    return total.astype(jnp.bfloat16)


def shifted(array, size, shift):
    return lax.ppermute(array, "narrow", [(i, (i + shift) % size) for i in range(size)])


def per_device(wide, narrow, hidden, grad_out, weight_base, block_scale):
    tokens_here, groups, slice_width = hidden.shape
    per_root = wide // narrow
    contract_last = (((1,), (1,)), ((), ()))
    blocks = [grad_out] + [shifted(grad_out, narrow, k) for k in range(1, narrow)]
    tokens_all = jnp.concatenate(blocks, axis=0)
    effective = apply_scales(weight_base, block_scale)

    flat = hidden.reshape(tokens_here, groups * slice_width)
    flats = [flat] + [shifted(flat, narrow, k) for k in range(1, narrow)]

    cut = tokens_all.shape[0] // RING_ROWS if RING_ROWS else 0
    rows_called = tokens_all.shape[0] - cut
    call_half = lax.dot_general(
        tokens_all[:rows_called], effective, contract_last, preferred_element_type=jnp.float32
    ).astype(jnp.bfloat16)
    call_sum = lax.psum_scatter(call_half, "wide", scatter_dimension=1, tiled=True)

    me_n = lax.axis_index("narrow")
    me_a = lax.axis_index("wide") // per_root
    me_b = lax.axis_index("wide") % per_root
    tokens_held, call_half = lax.optimization_barrier((tokens_all, call_half))
    cames = []
    for k in range(1, narrow):
        pairs = []
        for n in range(narrow):
            for b in range(per_root):
                source = (n * per_root + b) * narrow + n
                target = (((n + k) % narrow) * per_root + b) * narrow + n
                pairs.append((source, target))
        cames.append(lax.ppermute(tokens_held, ("wide", "narrow"), pairs))

    if cut:
        ring_half = lax.dot_general(
            tokens_held[-cut:], effective, contract_last, preferred_element_type=jnp.float32
        )
        ring_half, cames, flats = lax.optimization_barrier((ring_half, cames, flats))
        ring_sum = ring_reduce_scatter(ring_half, wide, slice_width)

    column = tokens_held
    for k in range(1, narrow):
        column = jnp.where((me_a - me_n) % narrow == k, cames[k - 1], column)
    pieces = [column]
    for k in range(1, per_root):
        pairs = [
            (a * per_root + b, a * per_root + (b + k) % per_root)
            for a in range(narrow)
            for b in range(per_root)
        ]
        pieces.append(lax.ppermute(column, "wide", pairs))
    columns_mine = jnp.concatenate(
        [jnp.stack(pieces)[(me_b - r) % per_root] if per_root > 2
         else jnp.where(me_b == r, pieces[0], pieces[-1]) for r in range(per_root)], axis=1
    )
    hidden_all = jnp.concatenate(flats, axis=0)
    product = lax.dot_general(
        columns_mine, hidden_all, (((0,), (0,)), ((), ())), preferred_element_type=jnp.float32
    )
    grad_weight = product.astype(jnp.bfloat16).reshape(product.shape[0], groups, slice_width)

    call_sum, grad_weight = lax.optimization_barrier((call_sum, grad_weight))
    summed = jnp.concatenate([call_sum, ring_sum], axis=0) if cut else call_sum
    parts = [summed[:tokens_here]]
    for k in range(1, narrow):
        parts.append(shifted(summed[k * tokens_here:(k + 1) * tokens_here], narrow, -k))
    stacked = jnp.stack(parts + parts, axis=1)
    grad_hidden = lax.dynamic_slice_in_dim(stacked, (narrow - me_n) % narrow, narrow, 1)
    return (grad_hidden, grad_weight)


def solution(mesh):
    wide, narrow = mesh.shape["wide"], mesh.shape["narrow"]

    def body(hidden, grad_out, weight_base, block_scale):
        return per_device(wide, narrow, hidden, grad_out, weight_base, block_scale)

    return jax.shard_map(
        body,
        mesh=mesh,
        in_specs=(
            P("narrow", None, "wide"),
            P("narrow", "wide"),
            P("narrow", "wide"),
            P("narrow", "wide"),
        ),
        out_specs=(P("narrow", None, "wide"), P("narrow", None, "wide")),
        check_vma=False,
    )
```
